128 devices in a mesh: dp: 1, row: 16 (over z, y), col: 8 (over x, core).
Axes of the slice: x: 4, y: 4, z: 4, core: 2. Of those that a mesh axis runs over, the one named last changes fastest.
Arguments:
- hidden: bfloat16 [128, 256, 2048], P(('dp', 'row', 'col'))
- positions: int32 [128, 256], P(('dp', 'row', 'col'))
- segments: int32 [128, 256], P(('dp', 'row', 'col'))
- ln_weight: bfloat16 [2, 2048], replicated
- w_qkv: bfloat16 [2, 2048, 6144], P(None, None, ('row', 'col'))
- w_out: bfloat16 [2, 2048, 2048], P(None, ('row', 'col'))
- w_gate: bfloat16 [2, 2048, 8192], P(None, None, ('row', 'col'))
- w_up: bfloat16 [2, 2048, 8192], P(None, None, ('row', 'col'))
- w_down: bfloat16 [2, 8192, 2048], P(None, ('row', 'col'))
Outputs:
- output 1: bfloat16 [128, 256, 2048], P(('dp', 'row', 'col'))
- output 2: bfloat16 [128, 2, 16, 256, 128], P(('dp', 'row', 'col'))
- output 3: bfloat16 [128, 2, 16, 256, 128], P(('dp', 'row', 'col'))
All inputs are finite; a program needn't handle non-finite values.
Results may differ from the reference program's by a relative error of at most 0.0126783.
Values are sent between devices in bfloat16 or wider.
A program may use at most 1 GiB of HBM per device.

```python
import jax
import jax.numpy as jnp
from jax import lax

LAYERS = 2
BATCH_ROWS = 128
SEQ_LEN = 256
MODEL_DIM = 2048
NUM_HEADS = 16
KV_HEADS = 16
HEAD_DIM = 128
FFN_DIM = 8192
SEG_BREAKS = 4
NORM_EPS = 1e-5
ROPE_BASE = 8000000.0


def draw_segments(seg_key):
    token_idx = jnp.arange(SEQ_LEN, dtype=jnp.int32)[None, :]
    rand_draws = jax.random.randint(seg_key, (BATCH_ROWS, SEQ_LEN), 0, SEQ_LEN)
    breaks = (rand_draws < SEG_BREAKS) & (token_idx > 0)
    segments = jnp.cumsum(breaks.astype(jnp.int32), axis=1).astype(jnp.int32)
    starts = lax.cummax(jnp.where(breaks, token_idx, 0), axis=1)
    positions = (token_idx - starts).astype(jnp.int32)
    return positions, segments


def setup_inputs(seed: int = 0, part: int = 0) -> dict:
    base_key = jax.random.key(seed)
    part_key = jax.random.fold_in(base_key, part)
    hidden_key, seg_key = jax.random.split(part_key)
    weight_keys = jax.random.split(base_key, 6)
    qkv_cols = (NUM_HEADS + 2 * KV_HEADS) * HEAD_DIM
    attn_cols = NUM_HEADS * HEAD_DIM
    hidden = jax.random.normal(hidden_key, (BATCH_ROWS, SEQ_LEN, MODEL_DIM), jnp.float32)
    positions, segments = draw_segments(seg_key)
    ln_weight = 1.0 + 0.3 * jax.random.normal(weight_keys[0], (LAYERS, MODEL_DIM), jnp.float32)
    w_qkv = jax.random.normal(weight_keys[1], (LAYERS, MODEL_DIM, qkv_cols), jnp.float32) * MODEL_DIM ** -0.5
    w_out = jax.random.normal(weight_keys[2], (LAYERS, attn_cols, MODEL_DIM), jnp.float32) * (4.0 * attn_cols ** -0.5)
    w_gate = jax.random.normal(weight_keys[3], (LAYERS, MODEL_DIM, FFN_DIM), jnp.float32) * MODEL_DIM ** -0.5
    w_up = jax.random.normal(weight_keys[4], (LAYERS, MODEL_DIM, FFN_DIM), jnp.float32) * MODEL_DIM ** -0.5
    w_down = jax.random.normal(weight_keys[5], (LAYERS, FFN_DIM, MODEL_DIM), jnp.float32) * (2.0 * FFN_DIM ** -0.5)
    return {
        "hidden": hidden.astype(jnp.bfloat16),
        "positions": positions,
        "segments": segments,
        "ln_weight": ln_weight.astype(jnp.bfloat16),
        "w_qkv": w_qkv.astype(jnp.bfloat16),
        "w_out": w_out.astype(jnp.bfloat16),
        "w_gate": w_gate.astype(jnp.bfloat16),
        "w_up": w_up.astype(jnp.bfloat16),
        "w_down": w_down.astype(jnp.bfloat16),
    }


def layer_norm(hidden_row, norm_gain):
    hidden_f = hidden_row.astype(jnp.float32)
    mean_val = jnp.mean(hidden_f, axis=-1, keepdims=True)
    centred = hidden_f - mean_val
    var_val = jnp.mean(centred * centred, axis=-1, keepdims=True)
    return (centred * lax.rsqrt(var_val + NORM_EPS) * norm_gain.astype(jnp.float32)).astype(jnp.bfloat16)


def rotary(heads_in, cos_tab, sin_tab):
    pair_view = heads_in.astype(jnp.float32).reshape(heads_in.shape[:-1] + (HEAD_DIM // 2, 2))
    even_part = pair_view[..., 0]
    odd_part = pair_view[..., 1]
    rotated = jnp.stack([even_part * cos_tab - odd_part * sin_tab, odd_part * cos_tab + even_part * sin_tab], axis=-1)
    return rotated.reshape(heads_in.shape).astype(jnp.bfloat16)


def one_layer(hidden_row, pos_row, seg_row, norm_gain, w_qkv, w_out, w_gate, w_up, w_down):
    group_size = NUM_HEADS // KV_HEADS
    q_cols = NUM_HEADS * HEAD_DIM
    kv_cols = KV_HEADS * HEAD_DIM
    normed = layer_norm(hidden_row, norm_gain)
    projected = jnp.dot(normed, w_qkv, preferred_element_type=jnp.float32).astype(jnp.bfloat16)
    inv_freq = ROPE_BASE ** (-2.0 * jnp.arange(HEAD_DIM // 2, dtype=jnp.float32) / HEAD_DIM)
    angles = pos_row.astype(jnp.float32)[:, None, None] * inv_freq
    cos_tab = jnp.cos(angles)
    sin_tab = jnp.sin(angles)
    queries = rotary(projected[:, :q_cols].reshape(SEQ_LEN, NUM_HEADS, HEAD_DIM), cos_tab, sin_tab)
    keys_rot = rotary(projected[:, q_cols:q_cols + kv_cols].reshape(SEQ_LEN, KV_HEADS, HEAD_DIM), cos_tab, sin_tab)
    values = projected[:, q_cols + kv_cols:].reshape(SEQ_LEN, KV_HEADS, HEAD_DIM)
    grouped = queries.reshape(SEQ_LEN, KV_HEADS, group_size, HEAD_DIM)
    scores = jnp.einsum("skgd,tkd->kgst", grouped.astype(jnp.float32), keys_rot.astype(jnp.float32)) * HEAD_DIM ** -0.5
    token_idx = jnp.arange(SEQ_LEN)
    allowed = (token_idx[None, :] <= token_idx[:, None]) & (seg_row[None, :] == seg_row[:, None])
    scores = jnp.where(allowed, scores, -1e30)
    attn_probs = jax.nn.softmax(scores, axis=-1).astype(jnp.bfloat16)
    attn_out = jnp.einsum("kgst,tkd->skgd", attn_probs.astype(jnp.float32), values.astype(jnp.float32))
    attn_out = attn_out.astype(jnp.bfloat16).reshape(SEQ_LEN, q_cols)
    gate_pre = jnp.dot(normed, w_gate, preferred_element_type=jnp.float32)
    up_proj = jnp.dot(normed, w_up, preferred_element_type=jnp.float32)
    activated = (jax.nn.silu(gate_pre) * up_proj).astype(jnp.bfloat16)
    summed = hidden_row.astype(jnp.float32) + jnp.dot(attn_out, w_out, preferred_element_type=jnp.float32) + jnp.dot(activated, w_down, preferred_element_type=jnp.float32)
    return summed.astype(jnp.bfloat16), keys_rot.transpose(1, 0, 2), values.transpose(1, 0, 2)


def reference(hidden, positions, segments, ln_weight, w_qkv, w_out, w_gate, w_up, w_down):
    def per_row(row_args):
        hidden_row, pos_row, seg_row = row_args

        def layer_step(carry_row, layer_args):
            new_row, key_row, value_row = one_layer(carry_row, pos_row, seg_row, *layer_args)
            return new_row, (key_row, value_row)

        final_row, (key_rows, value_rows) = lax.scan(layer_step, hidden_row, (ln_weight, w_qkv, w_out, w_gate, w_up, w_down))
        return final_row, key_rows, value_rows

    hidden_out, k_cache, v_cache = lax.map(per_row, (hidden, positions, segments))
    return hidden_out, k_cache, v_cache
```

```python
import jax
import jax.numpy as jnp
from jax import lax
from jax.sharding import PartitionSpec as P

HEAD_DIM = 128
NORM_EPS = 1e-5
ROPE_BASE = 8000000.0
UNIT = 16


def layer_norm(hidden, norm_gain):
    hidden_f = hidden.astype(jnp.float32)
    mean_val = jnp.mean(hidden_f, axis=-1, keepdims=True)
    centred = hidden_f - mean_val
    var_val = jnp.mean(centred * centred, axis=-1, keepdims=True)
    return (centred * lax.rsqrt(var_val + NORM_EPS) * norm_gain.astype(jnp.float32)).astype(jnp.bfloat16)


def rotary(heads_in, cos_tab, sin_tab):
    pair_view = heads_in.astype(jnp.float32).reshape(heads_in.shape[:-1] + (heads_in.shape[-1] // 2, 2))
    even_part = pair_view[..., 0]
    odd_part = pair_view[..., 1]
    rotated = jnp.stack([even_part * cos_tab - odd_part * sin_tab, odd_part * cos_tab + even_part * sin_tab], axis=-1)
    return rotated.reshape(heads_in.shape).astype(jnp.bfloat16)


def solution(mesh):
    n_row, n_col = mesh.shape["row"], mesh.shape["col"]
    n_x = n_col // 2
    group = n_row * n_col
    both = ("row", "col")
    tok_spec = P(("dp", "row", "col"))
    col_spec = P(None, None, both)
    row_spec = P(None, both, None)

    def shift(value, dx):
        return lax.ppermute(value, "col", [(2 * ((x + dx) % n_x) + c, 2 * x + c) for x in range(n_x) for c in range(2)])

    def swap(value):
        return lax.ppermute(value, "col", [(i, i ^ 1) for i in range(n_col)])

    def gather_rel(value):
        half = value.shape[-1] // 2
        up = shift(value, 1)
        down = shift(value, 3)
        far = jnp.concatenate([shift(up[..., :half], 1), shift(down[..., half:], 3)], axis=-1)
        mine = jnp.stack([value, up, down, far])
        other = swap(mine)
        return jnp.stack([mine, other], axis=1)

    def device_fn(hidden, positions, segments, ln_weight, w_qkv, w_out, w_gate, w_up, w_down):
        layers, seq = w_qkv.shape[0], hidden.shape[1]
        model = hidden.shape[2]
        my_col = lax.axis_index("col")
        my_x, my_core = my_col // 2, my_col % 2
        v_idx = UNIT * my_col + lax.axis_index("row")
        qkv_t = w_qkv.transpose(0, 2, 1).reshape(layers, 3, UNIT, model)
        got = []
        for i in range(3):
            perm = []
            for d in range(group):
                u = (3 * d + i) % group
                perm.append((d, n_col * (u % UNIT) + u // UNIT))
            got.append(lax.ppermute(qkv_t[:, i], both, perm))
        got = jnp.stack(got)
        units = [lax.dynamic_index_in_dim(got, (v_idx + 2 * t) % 3, 0, keepdims=False) for t in range(3)]
        out_rows = lax.ppermute(w_out, both, [(d, n_col * (d % UNIT) + d // UNIT) for d in range(group)])
        shard = jnp.concatenate(units + [w_gate.transpose(0, 2, 1), w_up.transpose(0, 2, 1), out_rows, w_down], axis=1)
        full = [lax.all_gather(shard[l], "row", axis=0) for l in range(layers)]

        ids = gather_rel(jnp.stack([positions[0], segments[0]]))
        ids = ids.reshape(n_col, 2, seq)
        inv_freq = ROPE_BASE ** (-2.0 * jnp.arange(HEAD_DIM // 2, dtype=jnp.float32) / HEAD_DIM)
        angles = ids[:, 0].astype(jnp.float32)[..., None, None] * inv_freq
        cos_tab, sin_tab = jnp.cos(angles), jnp.sin(angles)
        tok = jnp.arange(seq)
        allowed = (tok[None, :] <= tok[:, None])[None] & (ids[:, 1][:, :, None] == ids[:, 1][:, None, :])

        x = hidden[0]
        key_list, value_list = [], []
        for l in range(layers):
            w = full[l]
            w_q = w[:, :48].reshape(n_row, 3, UNIT, model)
            w_g = w[:, 48:112]
            w_u = w[:, 112:176]
            w_o = w[:, 176:192]
            w_d = w[:, 192:256]
            normed = layer_norm(x, ln_weight[l])
            rows = gather_rel(normed).reshape(n_col, seq, model)
            proj = jnp.einsum("bsd,rtud->btsru", rows, w_q, preferred_element_type=jnp.float32).astype(jnp.bfloat16)
            proj = proj.reshape(n_col, 3, seq, 2, HEAD_DIM)
            q = rotary(proj[:, 0], cos_tab, sin_tab)
            k = rotary(proj[:, 1], cos_tab, sin_tab)
            v = proj[:, 2]
            scores = jnp.einsum("bshd,bthd->bhst", q, k, preferred_element_type=jnp.float32) * HEAD_DIM ** -0.5
            scores = jnp.where(allowed[:, None], scores, -1e30)
            probs = jax.nn.softmax(scores, axis=-1).astype(jnp.bfloat16)
            o = jnp.einsum("bhst,bthd->bshd", probs, v, preferred_element_type=jnp.float32).astype(jnp.bfloat16)
            o = o.reshape(n_col, seq, n_row, UNIT)
            kv = jnp.stack([k, v]).transpose(1, 0, 3, 2, 4).reshape(n_x, 2, 2, 2, seq, HEAD_DIM)
            theirs = swap(kv[:, 1])
            kv = kv[:, 0]
            first = jnp.where(my_core == 0, kv, theirs)
            second = jnp.where(my_core == 0, theirs, kv)
            pair = jnp.concatenate([first, second], axis=2)
            kv_rel = jnp.stack([pair[0], shift(pair[2], 1), shift(pair[3], 2), shift(pair[1], 3)])
            kv_abs = lax.dynamic_slice_in_dim(jnp.concatenate([kv_rel, kv_rel]), (n_x - my_x) % n_x, n_x, 0)
            kv_abs = kv_abs.transpose(1, 0, 2, 3, 4).reshape(2, 2 * n_col, seq, HEAD_DIM)
            key_list.append(kv_abs[0])
            value_list.append(kv_abs[1])

            gate = jnp.einsum("bsd,rfd->bsrf", rows, w_g, preferred_element_type=jnp.float32)
            up = jnp.einsum("bsd,rfd->bsrf", rows, w_u, preferred_element_type=jnp.float32)
            act = (jax.nn.silu(gate) * up).astype(jnp.bfloat16)
            act = act.reshape(n_x, 2, seq, n_row, 64)
            o = o.reshape(n_x, 2, seq, n_row, UNIT)

            def partial(i):
                p = jnp.einsum("csrf,rfd->csd", act[i], w_d, preferred_element_type=jnp.float32)
                p = p + jnp.einsum("csru,rud->csd", o[i], w_o, preferred_element_type=jnp.float32)
                return p[0] + swap(p[1])

            half = model // 2
            s_up, s_down, s_far, s_own = partial(1), partial(2), partial(3), None
            plus = shift(s_down[:, :half], 3)
            minus = shift(s_up[:, half:], 1)
            plus = shift(plus + s_far[:, :half], 3)
            minus = shift(minus + s_far[:, half:], 1)
            plus = shift(plus + s_up[:, :half], 3)
            minus = shift(minus + s_down[:, half:], 1)
            s_own = partial(0)
            total = jnp.concatenate([plus, minus], axis=-1) + s_own
            x = (x.astype(jnp.float32) + total).astype(jnp.bfloat16)
        return x[None], jnp.stack(key_list)[None], jnp.stack(value_list)[None]

    return jax.shard_map(device_fn, mesh=mesh, in_specs=(tok_spec, tok_spec, tok_spec, P(), col_spec, row_spec, col_spec, col_spec, row_spec), out_specs=(tok_spec, tok_spec, tok_spec), check_vma=False)
```

```python
import jax
import jax.numpy as jnp
from jax import lax
from jax.experimental import pallas as pl
from jax.experimental.pallas import tpu as pltpu
from jax.sharding import PartitionSpec as P

HEAD_DIM = 128
NORM_EPS = 1e-5
ROPE_BASE = 8000000.0
UNIT = 16
SEQ = 256
HT = 128
DIM = 2048
MESH = pl.DeviceIdType.MESH
LANE = 128
SIDE = 1024
QUART = 512
PART = 32
NX = 4
LAST = 3
FAR = 6
GC = 8
GROUP = 128
UNITS = 4
INV3 = 43
OFFS = (0, 3, 7, 11)
CNTS = (3, 4, 4, 5)
ORDER = ((1, 0, 2, 3), (0, 1, 2, 3))
TWO = (0, 1)
F32 = jnp.float32
BF16 = jnp.bfloat16


def dot_nt(a, b):
    return lax.dot_general(a, b, (((1,), (1,)), ((), ())), preferred_element_type=F32)


def dot_nn(a, b):
    return lax.dot_general(a, b, (((1,), (0,)), ((), ())), preferred_element_type=F32)


def kernel(wq, wg, wu, wd, wo, hidden, gain, tab_own, out_ref, kc_ref, vc_ref,
           wbuf, stage, hbuf, tab, act, obuf, kvst, keep, psend, precv, rl, rr,
           u_recv, u_send, w_recv, w_send, w_own, w_cred, g_recv, g_send, t_recv, t_send, t_own,
           kv_recv, kv_send, kv_own, p_recv, p_send, r_recv, r_send):
    row = lax.axis_index("row")
    col = lax.axis_index("col")
    z, y = lax.div(row, NX), lax.rem(row, NX)
    x, c = lax.div(col, 2), lax.rem(col, 2)
    zs = [NX * lax.rem(z + d, NX) for d in range(NX)]
    ys = [lax.rem(y + d, NX) for d in range(NX)]
    xs = [2 * lax.rem(x + d, NX) for d in range(NX)]
    cs = [c, 1 - c]
    planes = [[a + b for b in ys] for a in zs]
    me = GC * row + col
    mine = UNIT * col + row

    def at(lin):
        return (0, lax.div(lin, GC), lax.rem(lin, GC))

    def dev_plane(dz, dy):
        return (0, planes[dz][dy], col)

    def dev_x(dx, dc):
        return (0, row, xs[dx] + cs[dc])

    plane_peers = [dev_plane(0, 1), dev_plane(0, LAST), dev_plane(1, 0), dev_plane(LAST, 0)]
    x_peers = [dev_x(o, e) for o in range(NX) for e in TWO if o + e > 0]

    kinds, goals, origins = [], [], []
    for i in range(UNITS):
        if i < 3:
            u = 3 * me + i
            kinds.append(lax.div(u, GROUP))
            v = lax.rem(u, GROUP)
            origins.append(lax.rem((mine + GROUP - i) * INV3, GROUP))
        else:
            kinds.append(3)
            v = me
            origins.append(mine)
        goals.append(GC * lax.rem(v, UNIT) + lax.div(v, UNIT))

    barrier = pltpu.get_barrier_semaphore()
    for peer in plane_peers + x_peers:
        pl.semaphore_signal(barrier, device_id=peer, device_id_type=MESH)
    arrivals = len(plane_peers) + len(x_peers)
    for lin, goal in zip(origins, goals):
        arrivals += jnp.where(goal == me, 0, 1)

        @pl.when(lin != me)
        def _():
            pl.semaphore_signal(barrier, device_id=at(lin), device_id_type=MESH)

    def unit_copies(i):
        src = wq.at[:, i] if i < 3 else wo
        dst = stage.at[:, kinds[i]]
        near = pltpu.make_async_copy(src, dst, u_recv)
        far = pltpu.make_async_remote_copy(
            src_ref=src, dst_ref=dst, send_sem=u_send.at[i], recv_sem=u_recv,
            device_id=at(goals[i]), device_id_type=MESH)
        return near, far

    def units_start():
        for i in range(UNITS):
            near, far = unit_copies(i)
            pl.when(goals[i] == me)(near.start)
            pl.when(goals[i] != me)(far.start)

    def units_wait():
        pltpu.make_async_copy(stage, stage, u_recv).wait()
        for i in range(UNITS):
            pl.when(goals[i] != me)(unit_copies(i)[1].wait_send)

    own = pl.ds(row * UNIT, UNIT)

    def own_copies(layer, k):
        if k == 0:
            pairs = [(stage.at[layer, pl.ds(0, 3)], wbuf.at[pl.ds(0, 3), own])]
        elif k == LAST:
            pairs = [(wd.at[layer], wbuf.at[pl.ds(OFFS[k], NX), own]), (stage.at[layer, LAST], wbuf.at[OFFS[k] + NX, own])]
        else:
            pairs = [((wg if k == 1 else wu).at[layer], wbuf.at[pl.ds(OFFS[k], NX), own])]
        return [pltpu.make_async_copy(a, b, w_own.at[k, i]) for i, (a, b) in enumerate(pairs)]

    def own_start(layer, k):
        for cp in own_copies(layer, k):
            cp.start()

    def own_wait(layer, k):
        for cp in own_copies(layer, k):
            cp.wait()

    own_start(0, 1)
    own_start(0, 2)
    tab_cp = pltpu.make_async_copy(tab_own, tab.at[0], t_own)
    tab_cp.start()

    def wcopy(k, half, msg, df, ds, part, tf, ts):
        slot = planes[ds][df] if half == 0 else planes[df][ds]
        lo, n = (half * SIDE, SIDE) if part is None else (half * SIDE + part * QUART, QUART)
        sl = wbuf.at[pl.ds(OFFS[k], CNTS[k]), pl.ds(slot * UNIT, UNIT), pl.ds(lo, n)]
        return pltpu.make_async_remote_copy(
            src_ref=sl, dst_ref=sl, send_sem=w_send.at[k], recv_sem=w_recv.at[k, half, msg],
            device_id=dev_plane(ts, tf) if half == 0 else dev_plane(tf, ts), device_id_type=MESH)

    def wsend(k, half, msg, df, ds, part, tf, ts):
        wcopy(k, half, msg, df, ds, part, tf, ts).start()

    def wwait(k, half, msg, df, ds, part):
        wcopy(k, half, msg, df, ds, part, 1, 0).wait_recv()

    def spread(k, half, d):
        wsend(k, half, NX * (d + 1), d, 0, None, 0, 1)
        wsend(k, half, NX * (d + 1) + 1, d, 0, None, 0, LAST)

    def e0(k):
        for half in TWO:
            wsend(k, half, 0, 0, 0, None, 1, 0)
            wsend(k, half, 1, 0, 0, None, LAST, 0)
        for half in TWO:
            spread(k, half, 0)

    def e1(k):
        for half in TWO:
            wwait(k, half, 0, LAST, 0, None)
            wwait(k, half, 1, 1, 0, None)
            wsend(k, half, 2, LAST, 0, 0, 1, 0)
            wsend(k, half, 3, 1, 0, 1, LAST, 0)
        for half in TWO:
            spread(k, half, LAST)
            spread(k, half, 1)

    def second(k, d):
        base = NX * (d + 1)
        for half in TWO:
            wwait(k, half, base, d, LAST, None)
            wwait(k, half, base + 1, d, 1, None)
            wsend(k, half, base + 2, d, LAST, 0, 0, 1)
            wsend(k, half, base + 3, d, 1, 1, 0, LAST)

    def e2(k):
        second(k, 0)

    def e3(k):
        for half in TWO:
            wwait(k, half, 2, 2, 0, 0)
            wwait(k, half, 3, 2, 0, 1)
            spread(k, half, 2)

    def e4(k):
        second(k, LAST)
        second(k, 1)

    def e5(k):
        second(k, 2)

    def e6(k):
        for half in TWO:
            for d in range(NX):
                wwait(k, half, NX * (d + 1) + 2, d, 2, 0)
                wwait(k, half, NX * (d + 1) + 3, d, 2, 1)
        total = wbuf.at[pl.ds(OFFS[k], CNTS[k]), pl.ds(0, SEQ - UNIT)]
        pltpu.make_async_remote_copy(
            src_ref=total, dst_ref=total, send_sem=w_send.at[k], recv_sem=w_recv.at[k, 0, 0],
            device_id=plane_peers[0], device_id_type=MESH).wait_send()

    def credit(k):
        for peer in plane_peers:
            pl.semaphore_signal(w_cred.at[k], device_id=peer, device_id_type=MESH)

    def begin(layer, k):
        if layer == 0:
            if k == 0:
                units_wait()
                own_start(0, 0)
                own_start(0, LAST)
        else:
            pl.semaphore_wait(w_cred.at[k], len(plane_peers))
            own_start(layer, k)
        own_wait(layer, k)
        e0(k)

    order = [(layer, k) for layer in TWO for k in ORDER[layer]]

    def stream():
        for i, (layer, k) in enumerate(order):
            yield e1(k)
            yield e2(k)
            yield begin(*order[i + 1]) if i + 1 < len(order) else None
            yield e3(k)
            yield e4(k)
            yield e5(k)
            yield e6(k)

    flow = stream()

    def w(n):
        for _ in range(n):
            next(flow)

    def gather_fns(buf, recv, send, rows, width):
        half0 = LANE * (width // LANE // 2)
        whole, lower, upper = (0, width), (0, half0), (half0, width - half0)
        sends = [
            (0, whole, FAR, 1, 0), (0, whole, 2, LAST, 0), (0, whole, 1, 0, 1),
            (FAR, lower, NX, 1, 0), (2, upper, NX, LAST, 0),
            (FAR, whole, FAR + 1, 0, 1), (2, whole, LAST, 0, 1), (NX, whole, NX + 1, 0, 1),
        ]

        def copy(msg, landed):
            slot, (lo, n), dst, dx, dc = sends[msg]
            return pltpu.make_async_remote_copy(
                src_ref=buf.at[dst if landed else slot, rows, pl.ds(lo, n)], dst_ref=buf.at[dst, rows, pl.ds(lo, n)],
                send_sem=send.at[msg], recv_sem=recv.at[msg], device_id=dev_x(dx, dc), device_id_type=MESH)

        def start(*msgs):
            for msg in msgs:
                copy(msg, False).start()

        def wait(*msgs):
            for msg in msgs:
                copy(msg, True).wait_recv()

        def f0():
            start(0, 1, 2)

        def f1():
            wait(0)
            start(3, 5)
            wait(1)
            start(4, 6)

        def f2():
            wait(2, 6)

        def f3():
            wait(3, 4)
            start(7)

        def f4():
            wait(5, 7)
            for msg in range(len(sends)):
                copy(msg, False).wait_send()

        return f0, f1, f2, f3, f4

    tok = [pl.ds(t * HT, HT) for t in TWO]
    g = [gather_fns(hbuf, g_recv.at[t], g_send.at[t], tok[t], DIM) for t in TWO]
    gt = gather_fns(tab, t_recv, t_send, pl.ds(0, SEQ), 3 * LANE)

    def norm(xf, layer):
        mean = jnp.mean(xf, axis=-1, keepdims=True)
        cen = xf - mean
        var = jnp.mean(cen * cen, axis=-1, keepdims=True)
        return (cen * lax.rsqrt(var + NORM_EPS) * gain[pl.ds(layer, 1), :]).astype(BF16)

    lane_even = lax.rem(lax.broadcasted_iota(jnp.int32, (HT, LANE), 1), 2) == 0

    def attend(t, p):
        nk = (t + 1) * HT

        def body(o, carry):
            h = hbuf[pl.ds(2 * o, 2), tok[t], :].reshape(2 * HT, DIM)
            q = dot_nt(h, wbuf[0]).astype(BF16)
            k = dot_nt(h, wbuf[1]).astype(BF16)
            v = dot_nt(h, wbuf[2]).astype(BF16)
            for e in TWO:
                slot = 2 * o + e
                cos = tab[slot, tok[t], pl.ds(0, LANE)]
                sin = tab[slot, tok[t], pl.ds(LANE, LANE)]
                pos = tab[slot, tok[t], pl.ds(2 * LANE, LANE)]

                def rope(val):
                    vf = val.astype(F32)
                    sw = jnp.where(lane_even, pltpu.roll(vf, LANE - 1, 1), pltpu.roll(vf, 1, 1))
                    return (vf * cos + sw * sin).astype(BF16)

                s_idx = lax.broadcasted_iota(jnp.int32, (HT, nk), 0) + t * HT
                t_idx = lax.broadcasted_iota(jnp.int32, (HT, nk), 1)
                first = s_idx.astype(F32) - (pos if t == 0 else jnp.concatenate([pos, pos], axis=1))
                ok = (t_idx <= s_idx) & (t_idx.astype(F32) >= first)
                for hd in TWO:
                    rs, cols = slice(e * HT, (e + 1) * HT), slice(hd * LANE, (hd + 1) * LANE)
                    kvst[slot, 0, hd, tok[t], :] = rope(k[rs, cols])
                    kvst[slot, 1, hd, tok[t], :] = v[rs, cols]
                    keys = kvst[slot, 0, hd, pl.ds(0, nk), :]
                    vals = kvst[slot, 1, hd, pl.ds(0, nk), :]
                    sc = dot_nt(rope(q[rs, cols]), keys) * (HEAD_DIM ** -0.5)
                    sc = jnp.where(ok, sc, -1e30)
                    ex = jnp.exp(sc - jnp.max(sc, axis=-1, keepdims=True))
                    pr = (ex / jnp.sum(ex, axis=-1, keepdims=True)).astype(BF16)
                    obuf[slot, tok[t], cols] = dot_nn(pr, vals).astype(BF16)
            return carry

        lax.fori_loop(2 * p, 2 * p + 2, body, 0)

    def mlp_in(t, p):
        slots = pl.ds(NX * p, NX)

        def body(j, carry):
            h = hbuf[slots, tok[t], :].reshape(NX * HT, DIM)
            gate = dot_nt(h, wbuf[OFFS[1] + j])
            up = dot_nt(h, wbuf[OFFS[2] + j])
            val = (gate * (1.0 / (1.0 + jnp.exp(-gate))) * up).astype(BF16)
            act[slots, tok[t], pl.ds(pl.multiple_of(j * SEQ, SEQ), SEQ)] = val.reshape(NX, HT, SEQ)
            return carry

        lax.fori_loop(0, NX, body, 0)

    sides = [pl.ds(side * SIDE, SIDE) for side in TWO]
    lead = (LAST, 1)

    def pcopy(t, side, o):
        return pltpu.make_async_remote_copy(
            src_ref=psend.at[o, :, sides[side]], dst_ref=precv.at[t, o, :, sides[side]], send_sem=p_send.at[side, o],
            recv_sem=p_recv.at[t, side, o], device_id=dev_x(0, 1), device_id_type=MESH)

    def mlp_out(t, side):
        def tile(n, carry):
            cols = pl.ds(pl.multiple_of(side * SIDE + n * SEQ, SEQ), SEQ)
            a = act[:, tok[t], :].reshape(GC * HT, SIDE)
            ov = obuf[:, tok[t], :].reshape(GC * HT, SEQ)
            wt = wbuf[pl.ds(OFFS[LAST], NX + 1), :, cols].reshape((NX + 1) * SEQ, SEQ)
            p = dot_nn(jnp.concatenate([a, ov], axis=1), wt).reshape(NX, 2, HT, SEQ)
            keep[t, :, :, cols] = p[:, 0]
            psend[:, :, cols] = p[:, 1]
            return carry

        lax.fori_loop(0, NX, tile, 0)
        for i in range(NX):
            pcopy(t, side, (lead[side], 2, 4 - lead[side], 0)[i]).start()

    def mlp_sent(t):
        for side in TWO:
            for o in range(NX):
                pcopy(t, side, o).wait_send()

    def rcopy(t, side, step, src):
        buf = rl if side == 0 else rr
        return pltpu.make_async_remote_copy(
            src_ref=src, dst_ref=buf.at[t, step], send_sem=r_send.at[side, t, step],
            recv_sem=r_recv.at[side, t, step], device_id=dev_x(lead[1 - side], 0), device_id_type=MESH)

    def ring0(t, side):
        o = lead[side]
        pcopy(t, side, o).wait_recv()
        keep[t, o, :, sides[side]] += precv[t, o, :, sides[side]]
        rcopy(t, side, 0, keep.at[t, o, :, sides[side]]).start()

    def ring(t, step):
        for side in TWO:
            buf = rl if side == 0 else rr
            o = 2 if step == 1 else lead[1 - side]
            pcopy(t, side, o).wait_recv()
            rcopy(t, side, step - 1, buf.at[t, step - 1]).wait_recv()
            buf[t, step - 1] += keep[t, o, :, sides[side]] + precv[t, o, :, sides[side]]
            rcopy(t, side, step, buf.at[t, step - 1]).start()

    def finish(t, layer):
        for side in TWO:
            pcopy(t, side, 0).wait_recv()
        for side in TWO:
            rcopy(t, side, 2, (rl if side == 0 else rr).at[t, 2]).wait_recv()

        def part(i, carry):
            rows = pl.ds(pl.multiple_of(i * PART, PART), PART)
            trows = pl.ds(pl.multiple_of(t * HT + i * PART, PART), PART)
            total = jnp.concatenate([rl[t, 2, rows], rr[t, 2, rows]], axis=1)
            total = total + (keep[t, 0, rows] + precv[t, 0, rows])
            xn = (out_ref[trows, :].astype(F32) + total).astype(BF16)
            out_ref[trows, :] = xn
            if layer == 0:
                hbuf[0, trows, :] = norm(xn.astype(F32), 1)
            return carry

        lax.fori_loop(0, HT // PART, part, 0)
        if layer == 0:
            g[t][0]()
        for side in TWO:
            for step in range(3):
                rcopy(t, side, step, rl.at[t, step]).wait_send()

    def kv_copies(layer, toks):
        return [
            pltpu.make_async_remote_copy(
                src_ref=kvst.at[2 * o + e, i, :, toks], dst_ref=ref.at[layer, pl.ds(2 * col, 2), toks], send_sem=kv_send,
                recv_sem=kv_recv.at[layer, i], device_id=dev_x(o, e), device_id_type=MESH)
            for o in range(NX) for e in TWO if o + e > 0 for i, ref in enumerate((kc_ref, vc_ref))
        ]

    def kv_local(layer):
        return [pltpu.make_async_copy(kvst.at[0, i], ref.at[layer, pl.ds(2 * col, 2)], kv_own.at[i]) for i, ref in enumerate((kc_ref, vc_ref))]

    def kv_start(layer, toks):
        for cp in kv_copies(layer, toks):
            cp.start()

    def kv_sent(layer):
        for cp in kv_local(layer):
            cp.start()
        total = kvst.at[pl.ds(1, GC - 1)]
        pltpu.make_async_remote_copy(src_ref=total, dst_ref=total, send_sem=kv_send, recv_sem=kv_recv.at[layer, 0],
                                     device_id=dev_x(0, 1), device_id_type=MESH).wait_send()
        for cp in kv_local(layer):
            cp.wait()

    x_cp = pltpu.make_async_copy(hidden, out_ref, t_own)
    tab_cp.wait()
    x_cp.start()
    x_cp.wait()

    def first_norm(i, carry):
        rows = pl.ds(pl.multiple_of(i * PART, PART), PART)
        hbuf[0, rows, :] = norm(out_ref[rows, :].astype(F32), 0)
        return carry

    lax.fori_loop(0, SEQ // PART, first_norm, 0)
    pl.semaphore_wait(barrier, arrivals)
    begin(0, 1)
    units_start()
    g[0][0]()
    g[1][0]()
    w(4)
    g[0][1]()
    w(2)
    g[1][1]()
    w(1)
    gt[0]()
    w(3)
    for fns in g:
        w(1)
        for fn in fns[2:]:
            fn()
    w(2)
    gt[1]()
    w(3)
    for fn in gt[2:]:
        fn()
    for t in TWO:
        for p in TWO:
            attend(t, p)
            w(1)
    credit(0)
    kv_start(0, pl.ds(0, SEQ))
    w(3)
    for t in TWO:
        for p in TWO:
            mlp_in(t, p)
            w(1)
    credit(1)
    credit(2)
    for t in TWO:
        for side in TWO:
            mlp_out(t, side)
            ring0(t, side)
            w(1)
        mlp_sent(t)
    credit(LAST)
    for (t, step), n in zip(((0, 1), (1, 1), (0, 2), (1, 2)), (1, 6, 3, 4)):
        w(n)
        ring(t, step)
    w(5)
    finish(0, 0)
    w(2)
    finish(1, 0)
    kv_sent(0)
    g[0][1]()
    g[0][2]()
    attend(0, 0)
    w(1)
    mlp_in(0, 0)
    w(1)
    g[1][1]()
    g[0][3]()
    w(1)
    g[0][4]()
    attend(0, 1)
    kv_start(1, tok[0])
    mlp_in(0, 1)
    for side in TWO:
        mlp_out(0, side)
        ring0(0, side)
    for fn in g[1][2:]:
        fn()
    attend(1, 0)
    ring(0, 1)
    attend(1, 1)
    mlp_in(1, 0)
    ring(0, 2)
    mlp_in(1, 1)
    mlp_sent(0)
    for side in TWO:
        mlp_out(1, side)
        ring0(1, side)
    finish(0, 1)
    ring(1, 1)
    ring(1, 2)
    kv_start(1, tok[1])
    finish(1, 1)
    mlp_sent(1)
    kv_sent(1)
    for layer in TWO:
        for i, ref in enumerate((kc_ref, vc_ref)):
            got = ref.at[layer, pl.ds(0, 2 * GC - 2)]
            pltpu.make_async_remote_copy(src_ref=got, dst_ref=got, send_sem=kv_send, recv_sem=kv_recv.at[layer, i],
                                         device_id=dev_x(0, 1), device_id_type=MESH).wait_recv()


def solution(mesh):
    tok_spec = P(("dp", "row", "col"))
    both = ("row", "col")
    col_spec = P(None, None, both)
    row_spec = P(None, both, None)

    def device_fn(hidden, positions, segments, ln_weight, w_qkv, w_out, w_gate, w_up, w_down):
        layers = w_qkv.shape[0]
        wq = w_qkv.transpose(0, 2, 1).reshape(layers, 3, UNIT, DIM)
        wg = w_gate.transpose(0, 2, 1).reshape(layers, NX, UNIT, DIM)
        wu = w_up.transpose(0, 2, 1).reshape(layers, NX, UNIT, DIM)
        wd = w_down.reshape(layers, NX, UNIT, DIM)

        inv_freq = ROPE_BASE ** (-2.0 * jnp.arange(HEAD_DIM // 2, dtype=F32) / HEAD_DIM)
        pos = positions[0].astype(F32)[:, None]
        angles = pos * inv_freq
        cos, sin = jnp.cos(angles), jnp.sin(angles)
        cos2 = jnp.stack([cos, cos], axis=-1).reshape(SEQ, HEAD_DIM)
        sin2 = jnp.stack([-sin, sin], axis=-1).reshape(SEQ, HEAD_DIM)
        tab_own = jnp.concatenate([cos2, sin2, jnp.broadcast_to(pos, (SEQ, HEAD_DIM))], axis=1)

        vm = pl.BlockSpec(memory_space=pltpu.VMEM)
        hb = pl.BlockSpec(memory_space=pl.ANY)
        dma = pltpu.SemaphoreType.DMA
        cache = jax.ShapeDtypeStruct((layers, 2 * GC, SEQ, HEAD_DIM), BF16)
        x_out, kc, vc = pl.pallas_call(
            kernel,
            out_shape=(jax.ShapeDtypeStruct((SEQ, DIM), BF16), cache, cache),
            in_specs=[hb] * 6 + [vm, hb],
            out_specs=(vm, hb, hb),
            scratch_shapes=[
                pltpu.VMEM((16, SEQ, DIM), BF16),
                pltpu.VMEM((2, UNITS, UNIT, DIM), BF16),
                pltpu.VMEM((GC, SEQ, DIM), BF16),
                pltpu.VMEM((GC, SEQ, 3 * LANE), F32),
                pltpu.VMEM((GC, SEQ, SIDE), BF16),
                pltpu.VMEM((GC, SEQ, SEQ), BF16),
                pltpu.VMEM((GC, 2, 2, SEQ, HEAD_DIM), BF16),
                pltpu.VMEM((2, NX, HT, DIM), F32),
                pltpu.VMEM((NX, HT, DIM), F32),
                pltpu.VMEM((2, NX, HT, DIM), F32),
                pltpu.VMEM((2, 3, HT, SIDE), F32),
                pltpu.VMEM((2, 3, HT, SIDE), F32),
                dma, dma((UNITS,)), dma((NX, 2, 20)), dma((NX,)), dma((NX, 2)), pltpu.SemaphoreType.REGULAR((NX,)),
                dma((2, GC)), dma((2, GC)), dma((GC,)), dma((GC,)), dma,
                dma((2, 2)), dma, dma((2,)), dma((2, 2, NX)), dma((2, NX)), dma((2, 2, 3)), dma((2, 2, 3)),
            ],
            compiler_params=pltpu.CompilerParams(collective_id=0, has_side_effects=True, vmem_limit_bytes=67043328),
        )(wq, wg, wu, wd, w_out, hidden[0], ln_weight.astype(F32), tab_own)
        return x_out[None], kc[None], vc[None]

    return jax.shard_map(device_fn, mesh=mesh, in_specs=(tok_spec, tok_spec, tok_spec, P(), col_spec, row_spec, col_spec, col_spec, row_spec), out_specs=(tok_spec, tok_spec, tok_spec), check_vma=False)
```

```python
import jax
import jax.numpy as jnp
from jax import lax
from jax.experimental import pallas as pl
from jax.experimental.pallas import tpu as pltpu
from jax.sharding import PartitionSpec as P

HEAD_DIM = 128
NORM_EPS = 1e-5
ROPE_BASE = 8000000.0
UNIT = 16
SEQ = 256
HT = 128
DIM = 2048
MESH = pl.DeviceIdType.MESH
LANE = 128
SIDE = 1024
QUART = 512
PART = 32
NX = 4
LAST = 3
FAR = 6
GC = 8
GROUP = 128
UNITS = 4
INV3 = 43
OFFS = (0, 3, 7, 11)
CNTS = (3, 4, 4, 5)
ORDER = ((1, 0, 2, 3), (1, 2, 0, 3))
TWO = (0, 1)
AHEAD = {0: (1,), 2: (2, 3), 7: (4, 5), 8: (6,), 10: (7,)}
F32 = jnp.float32
BF16 = jnp.bfloat16


def dot_nt(a, b):
    return lax.dot_general(a, b, (((1,), (1,)), ((), ())), preferred_element_type=F32)


def dot_nn(a, b):
    return lax.dot_general(a, b, (((1,), (0,)), ((), ())), preferred_element_type=F32)


def kernel(wq, wg, wu, wd, wo, hidden, gain, tab_own, out_ref, kc_ref, vc_ref, stage,
           wbuf, hbuf, tab, act, obuf, kvst, keep, psend, precv, rl, rr,
           u_recv, u_send, w_recv, w_send, w_own, w_cred, g_recv, g_send, t_recv, t_send, t_own,
           kv_recv, kv_send, kv_own, p_recv, p_send, r_recv, r_send):
    row = lax.axis_index("row")
    col = lax.axis_index("col")
    z, y = lax.div(row, NX), lax.rem(row, NX)
    x, c = lax.div(col, 2), lax.rem(col, 2)
    zs = [NX * lax.rem(z + d, NX) for d in range(NX)]
    ys = [lax.rem(y + d, NX) for d in range(NX)]
    xs = [2 * lax.rem(x + d, NX) for d in range(NX)]
    cs = [c, 1 - c]
    planes = [[a + b for b in ys] for a in zs]
    me = GC * row + col
    mine = UNIT * col + row

    def at(lin):
        return (0, lax.div(lin, GC), lax.rem(lin, GC))

    def dev_plane(dz, dy):
        return (0, planes[dz][dy], col)

    def dev_x(dx, dc):
        return (0, row, xs[dx] + cs[dc])

    plane_peers = [dev_plane(0, 1), dev_plane(0, LAST), dev_plane(1, 0), dev_plane(LAST, 0)]
    x_peers = [dev_x(o, e) for o in range(NX) for e in TWO if o + e > 0]

    kinds, goals, origins = [], [], []
    for i in range(UNITS):
        if i < 3:
            u = 3 * me + i
            kinds.append(lax.div(u, GROUP))
            v = lax.rem(u, GROUP)
            origins.append(lax.rem((mine + GROUP - i) * INV3, GROUP))
        else:
            kinds.append(3)
            v = me
            origins.append(mine)
        goals.append(GC * lax.rem(v, UNIT) + lax.div(v, UNIT))

    barrier = pltpu.get_barrier_semaphore()
    for peer in plane_peers + x_peers:
        pl.semaphore_signal(barrier, device_id=peer, device_id_type=MESH)
    arrivals = len(plane_peers) + len(x_peers)
    for lin, goal in zip(origins, goals):
        arrivals += jnp.where(goal == me, 0, 1)

        @pl.when(lin != me)
        def _():
            pl.semaphore_signal(barrier, device_id=at(lin), device_id_type=MESH)

    def unit_far(layer, i):
        return pltpu.make_async_remote_copy(
            src_ref=wq.at[layer, i] if i < 3 else wo.at[layer], dst_ref=stage.at[layer, kinds[i]],
            send_sem=u_send.at[layer, i], recv_sem=u_recv.at[layer], device_id=at(goals[i]), device_id_type=MESH)

    def units_start(layer):
        for i in range(UNITS):
            @pl.when(goals[i] == me)
            def _():
                pltpu.make_async_copy(wq.at[layer, i] if i < 3 else wo.at[layer], stage.at[layer, kinds[i]], u_recv.at[layer]).start()

            @pl.when(goals[i] != me)
            def _():
                unit_far(layer, i).start()

    def units_wait(layer):
        pltpu.make_async_copy(stage.at[layer], stage.at[layer], u_recv.at[layer]).wait()
        for i in range(UNITS):
            @pl.when(goals[i] != me)
            def _():
                unit_far(layer, i).wait_send()

    own = pl.ds(row * UNIT, UNIT)

    def own_copies(layer, k):
        if k == 0:
            pairs = [(stage.at[layer, pl.ds(0, 3)], wbuf.at[pl.ds(0, 3), own])]
        elif k == LAST:
            pairs = [(wd.at[layer], wbuf.at[pl.ds(OFFS[k], NX), own]), (stage.at[layer, LAST], wbuf.at[OFFS[k] + NX, own])]
        else:
            pairs = [((wg if k == 1 else wu).at[layer], wbuf.at[pl.ds(OFFS[k], NX), own])]
        return [pltpu.make_async_copy(a, b, w_own.at[k, i]) for i, (a, b) in enumerate(pairs)]

    def own_start(layer, k):
        for cp in own_copies(layer, k):
            cp.start()

    def own_wait(layer, k):
        for cp in own_copies(layer, k):
            cp.wait()

    own_start(0, 1)
    own_start(0, 2)
    tab_cp = pltpu.make_async_copy(tab_own, tab.at[0], t_own)
    tab_cp.start()

    def wcopy(k, half, msg, df, ds, part, tf, ts):
        slot = planes[ds][df] if half == 0 else planes[df][ds]
        lo, n = (half * SIDE, SIDE) if part is None else (half * SIDE + part * QUART, QUART)
        sl = wbuf.at[pl.ds(OFFS[k], CNTS[k]), pl.ds(slot * UNIT, UNIT), pl.ds(lo, n)]
        return pltpu.make_async_remote_copy(
            src_ref=sl, dst_ref=sl, send_sem=w_send.at[k], recv_sem=w_recv.at[k, half, msg],
            device_id=dev_plane(ts, tf) if half == 0 else dev_plane(tf, ts), device_id_type=MESH)

    def wsend(k, half, msg, df, ds, part, tf, ts):
        wcopy(k, half, msg, df, ds, part, tf, ts).start()

    def wwait(k, half, msg, df, ds, part):
        wcopy(k, half, msg, df, ds, part, 1, 0).wait_recv()

    def spread(k, half, d):
        wsend(k, half, NX * (d + 1), d, 0, None, 0, 1)
        wsend(k, half, NX * (d + 1) + 1, d, 0, None, 0, LAST)

    def e0(k):
        for half in TWO:
            wsend(k, half, 0, 0, 0, None, 1, 0)
            wsend(k, half, 1, 0, 0, None, LAST, 0)
        for half in TWO:
            spread(k, half, 0)

    def e1(k):
        for half in TWO:
            wwait(k, half, 0, LAST, 0, None)
            wwait(k, half, 1, 1, 0, None)
            wsend(k, half, 2, LAST, 0, 0, 1, 0)
            wsend(k, half, 3, 1, 0, 1, LAST, 0)
        for half in TWO:
            spread(k, half, LAST)
            spread(k, half, 1)

    def second(k, d):
        base = NX * (d + 1)
        for half in TWO:
            wwait(k, half, base, d, LAST, None)
            wwait(k, half, base + 1, d, 1, None)
            wsend(k, half, base + 2, d, LAST, 0, 0, 1)
            wsend(k, half, base + 3, d, 1, 1, 0, LAST)

    def e2(k):
        second(k, 0)

    def e3(k):
        for half in TWO:
            wwait(k, half, 2, 2, 0, 0)
            wwait(k, half, 3, 2, 0, 1)
            spread(k, half, 2)

    def e4(k):
        second(k, LAST)
        second(k, 1)

    def e5(k):
        second(k, 2)

    def e6(k):
        for half in TWO:
            for d in range(NX):
                wwait(k, half, NX * (d + 1) + 2, d, 2, 0)
                wwait(k, half, NX * (d + 1) + 3, d, 2, 1)
        total = wbuf.at[pl.ds(OFFS[k], CNTS[k]), pl.ds(0, SEQ - UNIT)]
        pltpu.make_async_remote_copy(
            src_ref=total, dst_ref=total, send_sem=w_send.at[k], recv_sem=w_recv.at[k, 0, 0],
            device_id=plane_peers[0], device_id_type=MESH).wait_send()

    def credit(k):
        for peer in plane_peers:
            pl.semaphore_signal(w_cred.at[k], device_id=peer, device_id_type=MESH)

    def begin(layer, k):
        if k == 0:
            units_wait(layer)
        if layer > 0:
            pl.semaphore_wait(w_cred.at[k], len(plane_peers))
        if layer > 0 or k in (0, LAST):
            own_start(layer, k)
        own_wait(layer, k)
        e0(k)

    order = [(layer, k) for layer in TWO for k in ORDER[layer]]

    def start_after(step):
        for j in AHEAD.get(step, ()):
            begin(*order[j])

    def stream():
        for i, (layer, k) in enumerate(order):
            yield e1(k)
            e2(k)
            yield start_after(2 * i)
            yield e3(k)
            yield e4(k)
            yield e5(k)
            e6(k)
            yield start_after(2 * i + 1)

    flow = stream()

    def w(n):
        for _ in range(n):
            next(flow)

    def gather_fns(buf, recv, send, rows, width):
        half0 = LANE * (width // LANE // 2)
        whole, lower, upper = (0, width), (0, half0), (half0, width - half0)
        sends = [
            (0, whole, FAR, 1, 0), (0, whole, 2, LAST, 0), (0, whole, 1, 0, 1),
            (FAR, lower, NX, 1, 0), (2, upper, NX, LAST, 0),
            (FAR, whole, FAR + 1, 0, 1), (2, whole, LAST, 0, 1), (NX, whole, NX + 1, 0, 1),
        ]

        def copy(msg, landed):
            slot, (lo, n), dst, dx, dc = sends[msg]
            return pltpu.make_async_remote_copy(
                src_ref=buf.at[dst if landed else slot, rows, pl.ds(lo, n)], dst_ref=buf.at[dst, rows, pl.ds(lo, n)],
                send_sem=send.at[msg], recv_sem=recv.at[msg], device_id=dev_x(dx, dc), device_id_type=MESH)

        def start(*msgs):
            for msg in msgs:
                copy(msg, False).start()

        def wait(*msgs):
            for msg in msgs:
                copy(msg, True).wait_recv()

        def f0():
            start(0, 1, 2)

        def f1():
            wait(0)
            start(3, 5)
            wait(1)
            start(4, 6)

        def f2():
            wait(2)

        def f3():
            wait(6)

        def f4():
            wait(3, 4)
            start(7)

        def f5():
            wait(5, 7)
            for msg in range(len(sends)):
                copy(msg, False).wait_send()

        return f0, f1, f2, f3, f4, f5

    tok = [pl.ds(t * HT, HT) for t in TWO]
    g = [gather_fns(hbuf, g_recv.at[t], g_send.at[t], tok[t], DIM) for t in TWO]
    gt = gather_fns(tab, t_recv, t_send, pl.ds(0, SEQ), 3 * LANE)

    def norm(xf, layer):
        mean = jnp.mean(xf, axis=-1, keepdims=True)
        cen = xf - mean
        var = jnp.mean(cen * cen, axis=-1, keepdims=True)
        return (cen * lax.rsqrt(var + NORM_EPS) * gain[pl.ds(layer, 1), :]).astype(BF16)

    lane_even = lax.rem(lax.broadcasted_iota(jnp.int32, (HT, LANE), 1), 2) == 0

    def attend(t, p, lo=0, hi=2):
        nk = (t + 1) * HT

        def body(o, carry):
            h = hbuf[pl.ds(2 * o, 2), tok[t], :].reshape(2 * HT, DIM)
            q = dot_nt(h, wbuf[0]).astype(BF16)
            k = dot_nt(h, wbuf[1]).astype(BF16)
            v = dot_nt(h, wbuf[2]).astype(BF16)
            old = [[kvst[2 * o + e, i, hd, tok[0], :] for i in TWO] for e in TWO for hd in TWO] if t > 0 else None
            outs = []
            for e in TWO:
                slot = 2 * o + e
                cos = tab[slot, tok[t], pl.ds(0, LANE)]
                sin = tab[slot, tok[t], pl.ds(LANE, LANE)]
                pos = tab[slot, tok[t], pl.ds(2 * LANE, LANE)]

                def rope(val):
                    vf = val.astype(F32)
                    sw = jnp.where(lane_even, pltpu.roll(vf, LANE - 1, 1), pltpu.roll(vf, 1, 1))
                    return (vf * cos + sw * sin).astype(BF16)

                s_idx = lax.broadcasted_iota(jnp.int32, (HT, nk), 0) + t * HT
                t_idx = lax.broadcasted_iota(jnp.int32, (HT, nk), 1)
                first = s_idx.astype(F32) - (pos if t == 0 else jnp.concatenate([pos, pos], axis=1))
                ok = (t_idx <= s_idx) & (t_idx.astype(F32) >= first)
                for hd in TWO:
                    rs, cols = slice(e * HT, (e + 1) * HT), slice(hd * LANE, (hd + 1) * LANE)
                    keys, vals = rope(k[rs, cols]), v[rs, cols]
                    kvst[slot, 0, hd, tok[t], :] = keys
                    kvst[slot, 1, hd, tok[t], :] = vals
                    if t > 0:
                        keys = jnp.concatenate([old[2 * e + hd][0], keys], axis=0)
                        vals = jnp.concatenate([old[2 * e + hd][1], vals], axis=0)
                    sc = dot_nt(rope(q[rs, cols]), keys) * (HEAD_DIM ** -0.5)
                    sc = jnp.where(ok, sc, -1e30)
                    ex = jnp.exp(sc - jnp.max(sc, axis=-1, keepdims=True))
                    pr = (ex / jnp.sum(ex, axis=-1, keepdims=True)).astype(BF16)
                    outs.append((slot, cols, dot_nn(pr, vals).astype(BF16)))
            for slot, cols, val in outs:
                obuf[slot, tok[t], cols] = val
            return carry

        lax.fori_loop(2 * p + lo, 2 * p + hi, body, 0)

    def mlp_in(t, p, lo=0, n=4):
        slots = pl.ds(NX * p + lo, n)

        def body(j, carry):
            h = hbuf[slots, tok[t], :].reshape(n * HT, DIM)
            gate = dot_nt(h, wbuf[OFFS[1] + j])
            up = dot_nt(h, wbuf[OFFS[2] + j])
            val = (gate * (1.0 / (1.0 + jnp.exp(-gate))) * up).astype(BF16)
            act[slots, tok[t], pl.ds(pl.multiple_of(j * SEQ, SEQ), SEQ)] = val.reshape(n, HT, SEQ)
            return carry

        lax.fori_loop(0, NX, body, 0)

    sides = [pl.ds(side * SIDE, SIDE) for side in TWO]
    lead = (LAST, 1)

    def pcopy(t, side, o):
        return pltpu.make_async_remote_copy(
            src_ref=psend.at[o, :, sides[side]], dst_ref=precv.at[t, o, :, sides[side]], send_sem=p_send.at[side, o],
            recv_sem=p_recv.at[t, side, o], device_id=dev_x(0, 1), device_id_type=MESH)

    def mlp_out(t, side):
        def tile(n, carry):
            cols = pl.ds(pl.multiple_of(side * SIDE + n * SEQ, SEQ), SEQ)
            a = act[:, tok[t], :].reshape(GC * HT, SIDE)
            ov = obuf[:, tok[t], :].reshape(GC * HT, SEQ)
            wt = wbuf[pl.ds(OFFS[LAST], NX + 1), :, cols].reshape((NX + 1) * SEQ, SEQ)
            p = dot_nn(jnp.concatenate([a, ov], axis=1), wt).reshape(NX, 2, HT, SEQ)
            keep[t, :, :, cols] = p[:, 0]
            psend[:, :, cols] = p[:, 1]
            return carry

        lax.fori_loop(0, NX, tile, 0)
        for i in range(NX):
            pcopy(t, side, (lead[side], 2, 4 - lead[side], 0)[i]).start()

    def mlp_sent(t):
        for side in TWO:
            for o in range(NX):
                pcopy(t, side, o).wait_send()

    def rcopy(t, side, step, src):
        buf = rl if side == 0 else rr
        return pltpu.make_async_remote_copy(
            src_ref=src, dst_ref=buf.at[t, step], send_sem=r_send.at[side, t, step],
            recv_sem=r_recv.at[side, t, step], device_id=dev_x(lead[1 - side], 0), device_id_type=MESH)

    def ring0(t, side):
        o = lead[side]
        pcopy(t, side, o).wait_recv()
        keep[t, o, :, sides[side]] += precv[t, o, :, sides[side]]
        rcopy(t, side, 0, keep.at[t, o, :, sides[side]]).start()

    def ring(t, step):
        for side in TWO:
            buf = rl if side == 0 else rr
            o = 2 if step == 1 else lead[1 - side]
            pcopy(t, side, o).wait_recv()
            rcopy(t, side, step - 1, buf.at[t, step - 1]).wait_recv()
            buf[t, step - 1] += keep[t, o, :, sides[side]] + precv[t, o, :, sides[side]]
            rcopy(t, side, step, buf.at[t, step - 1]).start()

    def finish(t, layer):
        for side in TWO:
            pcopy(t, side, 0).wait_recv()
        for side in TWO:
            rcopy(t, side, 2, (rl if side == 0 else rr).at[t, 2]).wait_recv()

        def part(i, carry):
            rows = pl.ds(pl.multiple_of(i * PART, PART), PART)
            trows = pl.ds(pl.multiple_of(t * HT + i * PART, PART), PART)
            total = jnp.concatenate([rl[t, 2, rows], rr[t, 2, rows]], axis=1)
            total = total + (keep[t, 0, rows] + precv[t, 0, rows])
            xn = (out_ref[trows, :].astype(F32) + total).astype(BF16)
            out_ref[trows, :] = xn
            if layer == 0:
                hbuf[0, trows, :] = norm(xn.astype(F32), 1)
            return carry

        lax.fori_loop(0, HT // PART, part, 0)
        if layer + t == 0:
            g[t][0]()
        for side in TWO:
            for step in range(3):
                rcopy(t, side, step, rl.at[t, step]).wait_send()

    def kv_copies(layer, toks, offs):
        return [
            pltpu.make_async_remote_copy(
                src_ref=kvst.at[2 * o + e, i, :, toks], dst_ref=ref.at[layer, pl.ds(2 * col, 2), toks], send_sem=kv_send,
                recv_sem=kv_recv.at[layer, i], device_id=dev_x(o, e), device_id_type=MESH)
            for o in offs for e in TWO if o + e > 0 for i, ref in enumerate((kc_ref, vc_ref))
        ]

    def kv_local(layer):
        return [pltpu.make_async_copy(kvst.at[0, i], ref.at[layer, pl.ds(2 * col, 2)], kv_own.at[i]) for i, ref in enumerate((kc_ref, vc_ref))]

    def kv_start(layer, toks, offs):
        for cp in kv_copies(layer, toks, offs):
            cp.start()

    def kv_sent(layer):
        for cp in kv_local(layer):
            cp.start()
        total = kvst.at[pl.ds(1, GC - 1)]
        pltpu.make_async_remote_copy(src_ref=total, dst_ref=total, send_sem=kv_send, recv_sem=kv_recv.at[layer, 0],
                                     device_id=dev_x(0, 1), device_id_type=MESH).wait_send()
        for cp in kv_local(layer):
            cp.wait()

    x_cp = pltpu.make_async_copy(hidden, out_ref, t_own)
    tab_cp.wait()
    x_cp.start()
    x_cp.wait()

    def first_norm(i, carry):
        rows = pl.ds(pl.multiple_of(i * PART, PART), PART)
        hbuf[0, rows, :] = norm(out_ref[rows, :].astype(F32), 0)
        return carry

    pl.semaphore_wait(barrier, arrivals)
    near, far = (0, 1, 3), (2,)
    (a0, a1, a2, a3, a4, a5), (b0, b1, *b_rest) = g
    t0, t1, *t_rest = gt
    begin(0, 1)
    units_start(0)
    lax.fori_loop(0, SEQ // PART, first_norm, 0)
    a0()
    b0()
    w(3)
    a1()
    w(2)
    b1()
    w(1)
    t0()
    w(2)
    for fns in g:
        w(1)
        for fn in fns[2:]:
            fn()
    w(2)
    t1()
    w(2)
    for fn in t_rest:
        fn()
    for t in TWO:
        for p in TWO:
            attend(t, p)
            w(1)
    credit(0)
    kv_start(0, pl.ds(0, SEQ), range(NX))
    w(2)
    for t in TWO:
        for p in TWO:
            mlp_in(t, p)
            if t + p < 2:
                w(1)
    credit(1)
    credit(2)
    w(1)
    for t in TWO:
        for side in TWO:
            mlp_out(t, side)
            ring0(t, side)
            if t + side == 0:
                units_start(1)
                w(1)
            else:
                w(1 - t)
        mlp_sent(t)
    credit(LAST)
    for (t, step), n in zip(((0, 1), (1, 1), (0, 2), (1, 2)), (3, 3, 3, 3)):
        w(n)
        ring(t, step)
    w(3)
    finish(0, 0)
    w(2)
    finish(1, 0)
    kv_sent(0)
    a2()
    attend(0, 0, 0, 1)
    mlp_in(0, 0, 0, 2)
    a1()
    b0()
    w(1)
    a3()
    attend(0, 0, 1, 2)
    mlp_in(0, 0, 2, 2)
    w(1)
    a4()
    a5()
    attend(0, 1)
    w(1)
    b1()
    mlp_in(0, 1)
    w(2)
    for side in TWO:
        mlp_out(0, side)
        ring0(0, side)
    kv_start(1, tok[0], near)
    for fn in b_rest:
        fn()
    attend(1, 0)
    attend(1, 1)
    ring(0, 1)
    kv_start(1, tok[0], far)
    mlp_in(1, 0)
    mlp_in(1, 1)
    mlp_sent(0)
    for side in TWO:
        mlp_out(1, side)
        ring0(1, side)
    ring(0, 2)
    ring(1, 1)
    kv_start(1, tok[1], near)
    finish(0, 1)
    ring(1, 2)
    kv_start(1, tok[1], far)
    finish(1, 1)
    mlp_sent(1)
    kv_sent(1)
    for layer in TWO:
        for i, ref in enumerate((kc_ref, vc_ref)):
            got = ref.at[layer, pl.ds(0, 2 * GC - 2)]
            pltpu.make_async_remote_copy(src_ref=got, dst_ref=got, send_sem=kv_send, recv_sem=kv_recv.at[layer, i],
                                         device_id=dev_x(0, 1), device_id_type=MESH).wait_recv()


def solution(mesh):
    tok_spec = P(("dp", "row", "col"))
    both = ("row", "col")
    col_spec = P(None, None, both)
    row_spec = P(None, both, None)

    def device_fn(hidden, positions, segments, ln_weight, w_qkv, w_out, w_gate, w_up, w_down):
        layers = w_qkv.shape[0]
        wq = w_qkv.transpose(0, 2, 1).reshape(layers, 3, UNIT, DIM)
        wg = w_gate.transpose(0, 2, 1).reshape(layers, NX, UNIT, DIM)
        wu = w_up.transpose(0, 2, 1).reshape(layers, NX, UNIT, DIM)
        wd = w_down.reshape(layers, NX, UNIT, DIM)

        inv_freq = ROPE_BASE ** (-2.0 * jnp.arange(HEAD_DIM // 2, dtype=F32) / HEAD_DIM)
        pos = positions[0].astype(F32)[:, None]
        angles = pos * inv_freq
        cos, sin = jnp.cos(angles), jnp.sin(angles)
        cos2 = jnp.stack([cos, cos], axis=-1).reshape(SEQ, HEAD_DIM)
        sin2 = jnp.stack([-sin, sin], axis=-1).reshape(SEQ, HEAD_DIM)
        tab_own = jnp.concatenate([cos2, sin2, jnp.broadcast_to(pos, (SEQ, HEAD_DIM))], axis=1)

        vm = pl.BlockSpec(memory_space=pltpu.VMEM)
        hb = pl.BlockSpec(memory_space=pl.ANY)
        dma, duo = pltpu.SemaphoreType.DMA, len(TWO)
        cache = jax.ShapeDtypeStruct((layers, 2 * GC, SEQ, HEAD_DIM), BF16)
        x_out, kc, vc, _ = pl.pallas_call(
            kernel,
            out_shape=(jax.ShapeDtypeStruct((SEQ, DIM), BF16), cache, cache, jax.ShapeDtypeStruct((layers, UNITS, UNIT, DIM), BF16)),
            in_specs=[hb] * 6 + [vm, hb],
            out_specs=(vm, hb, hb, hb),
            scratch_shapes=[
                pltpu.VMEM((16, SEQ, DIM), BF16),
                pltpu.VMEM((GC, SEQ, DIM), BF16),
                pltpu.VMEM((GC, SEQ, 3 * LANE), F32),
                pltpu.VMEM((GC, SEQ, SIDE), BF16),
                pltpu.VMEM((GC, SEQ, SEQ), BF16),
                pltpu.VMEM((GC, duo, duo, SEQ, HEAD_DIM), BF16),
                pltpu.VMEM((duo, NX, HT, DIM), F32),
                pltpu.VMEM((NX, HT, DIM), F32),
                pltpu.VMEM((duo, NX, HT, DIM), F32),
                pltpu.VMEM((duo, LAST, HT, SIDE), F32),
                pltpu.VMEM((duo, LAST, HT, SIDE), F32),
                dma((duo,)), dma((duo, UNITS)), dma((NX, duo, 20)), dma((NX,)), dma((NX, duo)), pltpu.SemaphoreType.REGULAR((NX,)),
                dma((duo, GC)), dma((duo, GC)), dma((GC,)), dma((GC,)), dma,
                dma((duo, duo)), dma, dma((duo,)), dma((duo, duo, NX)), dma((duo, NX)), dma((duo, duo, LAST)), dma((duo, duo, LAST)),
            ],
            compiler_params=pltpu.CompilerParams(collective_id=0, has_side_effects=True, vmem_limit_bytes=67043328),
        )(wq, wg, wu, wd, w_out, hidden[0], ln_weight.astype(F32), tab_own)
        return x_out[None], kc[None], vc[None]

    return jax.shard_map(device_fn, mesh=mesh, in_specs=(tok_spec, tok_spec, tok_spec, P(), col_spec, row_spec, col_spec, col_spec, row_spec), out_specs=(tok_spec, tok_spec, tok_spec), check_vma=False)
```

```python
import jax
import jax.numpy as jnp
from jax import lax
from jax.experimental import pallas as pl
from jax.experimental.pallas import tpu as pltpu
from jax.sharding import PartitionSpec as P

HEAD_DIM = 128
NORM_EPS = 1e-5
ROPE_BASE = 8000000.0
UNIT = 16
SEQ = 256
HT = 128
DIM = 2048
MESH = pl.DeviceIdType.MESH
LANE = 128
SIDE = 1024
QUART = 512
PART = 32
NX = 4
LAST = 3
FAR = 6
GC = 8
GROUP = 128
UNITS = 4
INV3 = 43
OFFS = (0, 3, 7, 11)
CNTS = (3, 4, 4, 5)
ORDER = ((1, 0, 2, 3), (1, 2, 0, 3))
TWO = (0, 1)
AHEAD = {0: (1,), 2: (2,), 4: (3,), 7: (4,), 8: (5,), 10: (6,), 12: (7,)}
F32 = jnp.float32
BF16 = jnp.bfloat16


def dot_nt(a, b):
    return lax.dot_general(a, b, (((1,), (1,)), ((), ())), preferred_element_type=F32)


def dot_nn(a, b):
    return lax.dot_general(a, b, (((1,), (0,)), ((), ())), preferred_element_type=F32)


def kernel(wq, wg, wu, wd, wo, hidden, gain, tab_own, out_ref, kc_ref, vc_ref, stage,
           wbuf, hbuf, tab, act, obuf, kvst, keep, psend, precv, rl, rr,
           u_recv, u_send, w_recv, w_send, w_own, w_cred, g_recv, g_send, t_recv, t_send, t_own,
           kv_recv, kv_send, kv_own, p_recv, p_send, r_recv, r_send):
    row = lax.axis_index("row")
    col = lax.axis_index("col")
    z, y = lax.div(row, NX), lax.rem(row, NX)
    x, c = lax.div(col, 2), lax.rem(col, 2)
    zs = [NX * lax.rem(z + d, NX) for d in range(NX)]
    ys = [lax.rem(y + d, NX) for d in range(NX)]
    xs = [2 * lax.rem(x + d, NX) for d in range(NX)]
    cs = [c, 1 - c]
    planes = [[a + b for b in ys] for a in zs]
    me = GC * row + col
    mine = UNIT * col + row

    def at(lin):
        return (0, lax.div(lin, GC), lax.rem(lin, GC))

    def dev_plane(dz, dy):
        return (0, planes[dz][dy], col)

    def dev_x(dx, dc):
        return (0, row, xs[dx] + cs[dc])

    plane_peers = [dev_plane(0, 1), dev_plane(0, LAST), dev_plane(1, 0), dev_plane(LAST, 0)]
    x_peers = [dev_x(o, e) for o in range(NX) for e in TWO if o + e > 0]

    kinds, goals, origins = [], [], []
    for i in range(UNITS):
        if i < 3:
            u = 3 * me + i
            kinds.append(lax.div(u, GROUP))
            v = lax.rem(u, GROUP)
            origins.append(lax.rem((mine + GROUP - i) * INV3, GROUP))
        else:
            kinds.append(3)
            v = me
            origins.append(mine)
        goals.append(GC * lax.rem(v, UNIT) + lax.div(v, UNIT))

    barrier = pltpu.get_barrier_semaphore()
    for peer in plane_peers + x_peers:
        pl.semaphore_signal(barrier, device_id=peer, device_id_type=MESH)
    arrivals = len(plane_peers) + len(x_peers)
    for lin, goal in zip(origins, goals):
        arrivals += jnp.where(goal == me, 0, 1)

        @pl.when(lin != me)
        def _():
            pl.semaphore_signal(barrier, device_id=at(lin), device_id_type=MESH)

    def unit_far(layer, i):
        return pltpu.make_async_remote_copy(
            src_ref=wq.at[layer, i] if i < 3 else wo.at[layer], dst_ref=stage.at[layer, kinds[i]],
            send_sem=u_send.at[layer, i], recv_sem=u_recv.at[layer], device_id=at(goals[i]), device_id_type=MESH)

    def units_start(layer):
        for i in range(UNITS):
            @pl.when(goals[i] == me)
            def _():
                pltpu.make_async_copy(wq.at[layer, i] if i < 3 else wo.at[layer], stage.at[layer, kinds[i]], u_recv.at[layer]).start()

            @pl.when(goals[i] != me)
            def _():
                unit_far(layer, i).start()

    def units_wait(layer):
        pltpu.make_async_copy(stage.at[layer], stage.at[layer], u_recv.at[layer]).wait()
        for i in range(UNITS):
            @pl.when(goals[i] != me)
            def _():
                unit_far(layer, i).wait_send()

    own = pl.ds(row * UNIT, UNIT)

    def own_copies(layer, k):
        if k == 0:
            pairs = [(stage.at[layer, pl.ds(0, 3)], wbuf.at[pl.ds(0, 3), own])]
        elif k == LAST:
            pairs = [(wd.at[layer], wbuf.at[pl.ds(OFFS[k], NX), own]), (stage.at[layer, LAST], wbuf.at[OFFS[k] + NX, own])]
        else:
            pairs = [((wg if k == 1 else wu).at[layer], wbuf.at[pl.ds(OFFS[k], NX), own])]
        return [pltpu.make_async_copy(a, b, w_own.at[k, i]) for i, (a, b) in enumerate(pairs)]

    def own_start(layer, k):
        for cp in own_copies(layer, k):
            cp.start()

    def own_wait(layer, k):
        for cp in own_copies(layer, k):
            cp.wait()

    own_start(0, 1)
    own_start(0, 2)
    tab_cp = pltpu.make_async_copy(tab_own, tab.at[0], t_own)
    tab_cp.start()

    def wcopy(k, half, msg, df, ds, part, tf, ts):
        slot = planes[ds][df] if half == 0 else planes[df][ds]
        lo, n = (half * SIDE, SIDE) if part is None else (half * SIDE + part * QUART, QUART)
        sl = wbuf.at[pl.ds(OFFS[k], CNTS[k]), pl.ds(slot * UNIT, UNIT), pl.ds(lo, n)]
        return pltpu.make_async_remote_copy(
            src_ref=sl, dst_ref=sl, send_sem=w_send.at[k], recv_sem=w_recv.at[k, half, msg],
            device_id=dev_plane(ts, tf) if half == 0 else dev_plane(tf, ts), device_id_type=MESH)

    def wsend(k, half, msg, df, ds, part, tf, ts):
        wcopy(k, half, msg, df, ds, part, tf, ts).start()

    def wwait(k, half, msg, df, ds, part):
        wcopy(k, half, msg, df, ds, part, 1, 0).wait_recv()

    def spread(k, half, d):
        wsend(k, half, NX * (d + 1), d, 0, None, 0, 1)
        wsend(k, half, NX * (d + 1) + 1, d, 0, None, 0, LAST)

    def e0(k):
        for half in TWO:
            wsend(k, half, 0, 0, 0, None, 1, 0)
            wsend(k, half, 1, 0, 0, None, LAST, 0)
        for half in TWO:
            spread(k, half, 0)

    def e1(k):
        for half in TWO:
            wwait(k, half, 0, LAST, 0, None)
            wwait(k, half, 1, 1, 0, None)
            wsend(k, half, 2, LAST, 0, 0, 1, 0)
            wsend(k, half, 3, 1, 0, 1, LAST, 0)
        for half in TWO:
            spread(k, half, LAST)
            spread(k, half, 1)

    def second(k, d):
        base = NX * (d + 1)
        for half in TWO:
            wwait(k, half, base, d, LAST, None)
            wwait(k, half, base + 1, d, 1, None)
            wsend(k, half, base + 2, d, LAST, 0, 0, 1)
            wsend(k, half, base + 3, d, 1, 1, 0, LAST)

    def e2(k):
        second(k, 0)

    def e3(k):
        for half in TWO:
            wwait(k, half, 2, 2, 0, 0)
            wwait(k, half, 3, 2, 0, 1)
            spread(k, half, 2)

    def e4(k):
        second(k, LAST)
        second(k, 1)

    def e5(k):
        second(k, 2)

    def e6(k):
        for half in TWO:
            for d in range(NX):
                wwait(k, half, NX * (d + 1) + 2, d, 2, 0)
                wwait(k, half, NX * (d + 1) + 3, d, 2, 1)
        total = wbuf.at[pl.ds(OFFS[k], CNTS[k]), pl.ds(0, SEQ - UNIT)]
        pltpu.make_async_remote_copy(
            src_ref=total, dst_ref=total, send_sem=w_send.at[k], recv_sem=w_recv.at[k, 0, 0],
            device_id=plane_peers[0], device_id_type=MESH).wait_send()

    def credit(k):
        for peer in plane_peers:
            pl.semaphore_signal(w_cred.at[k], device_id=peer, device_id_type=MESH)

    def begin(layer, k):
        if k == 0:
            units_wait(layer)
        if layer > 0:
            pl.semaphore_wait(w_cred.at[k], len(plane_peers))
        if layer > 0 or k in (0, LAST):
            own_start(layer, k)
        own_wait(layer, k)
        e0(k)

    order = [(layer, k) for layer in TWO for k in ORDER[layer]]

    def start_after(step):
        for j in AHEAD.get(step, ()):
            begin(*order[j])

    def stream():
        for i, (layer, k) in enumerate(order):
            yield e1(k)
            e2(k)
            yield start_after(2 * i)
            yield e3(k)
            yield e4(k)
            yield e5(k)
            e6(k)
            yield start_after(2 * i + 1)

    flow = stream()

    def w(n):
        for _ in range(n):
            next(flow)

    def gather_fns(buf, recv, send, rows, width):
        half0 = LANE * (width // LANE // 2)
        whole, lower, upper = (0, width), (0, half0), (half0, width - half0)
        sends = [
            (0, whole, FAR, 1, 0), (0, whole, 2, LAST, 0), (0, whole, 1, 0, 1),
            (FAR, lower, NX, 1, 0), (2, upper, NX, LAST, 0),
            (FAR, whole, FAR + 1, 0, 1), (2, whole, LAST, 0, 1), (NX, whole, NX + 1, 0, 1),
        ]

        def copy(msg, landed):
            slot, (lo, n), dst, dx, dc = sends[msg]
            return pltpu.make_async_remote_copy(
                src_ref=buf.at[dst if landed else slot, rows, pl.ds(lo, n)], dst_ref=buf.at[dst, rows, pl.ds(lo, n)],
                send_sem=send.at[msg], recv_sem=recv.at[msg], device_id=dev_x(dx, dc), device_id_type=MESH)

        def start(*msgs):
            for msg in msgs:
                copy(msg, False).start()

        def wait(*msgs):
            for msg in msgs:
                copy(msg, True).wait_recv()

        def f0():
            start(0, 1, 2)

        def f1():
            wait(0)
            start(3, 5)
            wait(1)
            start(4, 6)

        def f2():
            wait(2)

        def f3():
            wait(6)

        def f4():
            wait(3, 4)
            start(7)

        def f5():
            wait(5, 7)
            for msg in range(len(sends)):
                copy(msg, False).wait_send()

        return f0, f1, f2, f3, f4, f5

    tok = [pl.ds(t * HT, HT) for t in TWO]
    g = [gather_fns(hbuf, g_recv.at[t], g_send.at[t], tok[t], DIM) for t in TWO]
    gt = gather_fns(tab, t_recv, t_send, pl.ds(0, SEQ), 3 * LANE)

    def norm(xf, layer):
        mean = jnp.mean(xf, axis=-1, keepdims=True)
        cen = xf - mean
        var = jnp.mean(cen * cen, axis=-1, keepdims=True)
        return (cen * lax.rsqrt(var + NORM_EPS) * gain[pl.ds(layer, 1), :]).astype(BF16)

    lane_even = lax.rem(lax.broadcasted_iota(jnp.int32, (HT, LANE), 1), 2) == 0

    def attend(t, p, lo=0, hi=2):
        nk = (t + 1) * HT

        def body(o, carry):
            h = hbuf[pl.ds(2 * o, 2), tok[t], :].reshape(2 * HT, DIM)
            q = dot_nt(h, wbuf[0]).astype(BF16)
            k = dot_nt(h, wbuf[1]).astype(BF16)
            v = dot_nt(h, wbuf[2]).astype(BF16)
            old = [[kvst[2 * o + e, i, hd, tok[0], :] for i in TWO] for e in TWO for hd in TWO] if t > 0 else None
            outs = []
            for e in TWO:
                slot = 2 * o + e
                cos = tab[slot, tok[t], pl.ds(0, LANE)]
                sin = tab[slot, tok[t], pl.ds(LANE, LANE)]
                pos = tab[slot, tok[t], pl.ds(2 * LANE, LANE)]

                def rope(val):
                    vf = val.astype(F32)
                    sw = jnp.where(lane_even, pltpu.roll(vf, LANE - 1, 1), pltpu.roll(vf, 1, 1))
                    return (vf * cos + sw * sin).astype(BF16)

                s_idx = lax.broadcasted_iota(jnp.int32, (HT, nk), 0) + t * HT
                t_idx = lax.broadcasted_iota(jnp.int32, (HT, nk), 1)
                first = s_idx.astype(F32) - (pos if t == 0 else jnp.concatenate([pos, pos], axis=1))
                ok = (t_idx <= s_idx) & (t_idx.astype(F32) >= first)
                for hd in TWO:
                    rs, cols = slice(e * HT, (e + 1) * HT), slice(hd * LANE, (hd + 1) * LANE)
                    keys, vals = rope(k[rs, cols]), v[rs, cols]
                    kvst[slot, 0, hd, tok[t], :] = keys
                    kvst[slot, 1, hd, tok[t], :] = vals
                    if t > 0:
                        keys = jnp.concatenate([old[2 * e + hd][0], keys], axis=0)
                        vals = jnp.concatenate([old[2 * e + hd][1], vals], axis=0)
                    sc = dot_nt(rope(q[rs, cols]), keys) * (HEAD_DIM ** -0.5)
                    sc = jnp.where(ok, sc, -1e30)
                    ex = jnp.exp(sc - jnp.max(sc, axis=-1, keepdims=True))
                    pr = (ex / jnp.sum(ex, axis=-1, keepdims=True)).astype(BF16)
                    outs.append((slot, cols, dot_nn(pr, vals).astype(BF16)))
            for slot, cols, val in outs:
                obuf[slot, tok[t], cols] = val
            return carry

        lax.fori_loop(2 * p + lo, 2 * p + hi, body, 0)

    def mlp_in(t, p, lo=0, n=4):
        slots = pl.ds(NX * p + lo, n)

        def body(j, carry):
            h = hbuf[slots, tok[t], :].reshape(n * HT, DIM)
            gate = dot_nt(h, wbuf[OFFS[1] + j])
            up = dot_nt(h, wbuf[OFFS[2] + j])
            val = (gate * (1.0 / (1.0 + jnp.exp(-gate))) * up).astype(BF16)
            act[slots, tok[t], pl.ds(pl.multiple_of(j * SEQ, SEQ), SEQ)] = val.reshape(n, HT, SEQ)
            return carry

        lax.fori_loop(0, NX, body, 0)

    sides = [pl.ds(side * SIDE, SIDE) for side in TWO]
    lead = (LAST, 1)

    def pcopy(t, side, o):
        return pltpu.make_async_remote_copy(
            src_ref=psend.at[o, :, sides[side]], dst_ref=precv.at[t, o, :, sides[side]], send_sem=p_send.at[side, o],
            recv_sem=p_recv.at[t, side, o], device_id=dev_x(0, 1), device_id_type=MESH)

    def mlp_out(t, side):
        def tile(n, carry):
            cols = pl.ds(pl.multiple_of(side * SIDE + n * SEQ, SEQ), SEQ)
            a = act[:, tok[t], :].reshape(GC * HT, SIDE)
            ov = obuf[:, tok[t], :].reshape(GC * HT, SEQ)
            wt = wbuf[pl.ds(OFFS[LAST], NX + 1), :, cols].reshape((NX + 1) * SEQ, SEQ)
            p = dot_nn(jnp.concatenate([a, ov], axis=1), wt).reshape(NX, 2, HT, SEQ)
            keep[t, :, :, cols] = p[:, 0]
            psend[:, :, cols] = p[:, 1]
            return carry

        lax.fori_loop(0, NX, tile, 0)
        for i in range(NX):
            pcopy(t, side, (lead[side], 2, 4 - lead[side], 0)[i]).start()

    def mlp_sent(t):
        for side in TWO:
            for o in range(NX):
                pcopy(t, side, o).wait_send()

    def rcopy(t, side, step, src):
        buf = rl if side == 0 else rr
        return pltpu.make_async_remote_copy(
            src_ref=src, dst_ref=buf.at[t, step], send_sem=r_send.at[side, t, step],
            recv_sem=r_recv.at[side, t, step], device_id=dev_x(lead[1 - side], 0), device_id_type=MESH)

    def ring0(t, side):
        o = lead[side]
        pcopy(t, side, o).wait_recv()
        keep[t, o, :, sides[side]] += precv[t, o, :, sides[side]]
        rcopy(t, side, 0, keep.at[t, o, :, sides[side]]).start()

    def ring(t, step):
        for side in TWO:
            buf = rl if side == 0 else rr
            o = 2 if step == 1 else lead[1 - side]
            pcopy(t, side, o).wait_recv()
            rcopy(t, side, step - 1, buf.at[t, step - 1]).wait_recv()
            buf[t, step - 1] += keep[t, o, :, sides[side]] + precv[t, o, :, sides[side]]
            rcopy(t, side, step, buf.at[t, step - 1]).start()

    def finish(t, layer):
        for side in TWO:
            pcopy(t, side, 0).wait_recv()
        for side in TWO:
            rcopy(t, side, 2, (rl if side == 0 else rr).at[t, 2]).wait_recv()

        def part(i, carry):
            rows = pl.ds(pl.multiple_of(i * PART, PART), PART)
            trows = pl.ds(pl.multiple_of(t * HT + i * PART, PART), PART)
            total = jnp.concatenate([rl[t, 2, rows], rr[t, 2, rows]], axis=1)
            total = total + (keep[t, 0, rows] + precv[t, 0, rows])
            xn = (out_ref[trows, :].astype(F32) + total).astype(BF16)
            out_ref[trows, :] = xn
            if layer == 0:
                hbuf[0, trows, :] = norm(xn.astype(F32), 1)
            return carry

        lax.fori_loop(0, HT // PART, part, 0)
        if layer + t == 0:
            g[t][0]()
        for side in TWO:
            for step in range(3):
                rcopy(t, side, step, rl.at[t, step]).wait_send()

    def kv_copies(layer, toks, offs):
        return [
            pltpu.make_async_remote_copy(
                src_ref=kvst.at[2 * o + e, i, :, toks], dst_ref=ref.at[layer, pl.ds(2 * col, 2), toks], send_sem=kv_send,
                recv_sem=kv_recv.at[layer, i], device_id=dev_x(o, e), device_id_type=MESH)
            for o in offs for e in TWO if o + e > 0 for i, ref in enumerate((kc_ref, vc_ref))
        ]

    def kv_local(layer):
        return [pltpu.make_async_copy(kvst.at[0, i], ref.at[layer, pl.ds(2 * col, 2)], kv_own.at[i]) for i, ref in enumerate((kc_ref, vc_ref))]

    def kv_start(layer, toks, offs):
        for cp in kv_copies(layer, toks, offs):
            cp.start()

    def kv_sent(layer):
        for cp in kv_local(layer):
            cp.start()
        total = kvst.at[pl.ds(1, GC - 1)]
        pltpu.make_async_remote_copy(src_ref=total, dst_ref=total, send_sem=kv_send, recv_sem=kv_recv.at[layer, 0],
                                     device_id=dev_x(0, 1), device_id_type=MESH).wait_send()
        for cp in kv_local(layer):
            cp.wait()

    x_cp = pltpu.make_async_copy(hidden, out_ref, t_own)
    tab_cp.wait()
    x_cp.start()
    x_cp.wait()

    def first_norm(i, carry):
        rows = pl.ds(pl.multiple_of(i * PART, PART), PART)
        hbuf[0, rows, :] = norm(out_ref[rows, :].astype(F32), 0)
        return carry

    pl.semaphore_wait(barrier, arrivals)
    near, far = (0, 1, 3), (2,)
    (a0, a1, a2, a3, a4, a5), (b0, b1, *b_rest) = g
    t0, t1, *t_rest = gt
    begin(0, 1)
    units_start(0)
    lax.fori_loop(0, SEQ // PART, first_norm, 0)
    a0()
    b0()
    w(3)
    a1()
    w(2)
    b1()
    w(1)
    t0()
    w(2)
    for fns in g:
        w(1)
        for fn in fns[2:]:
            fn()
    w(2)
    t1()
    w(2)
    for fn in t_rest:
        fn()
    for t in TWO:
        for p in TWO:
            attend(t, p)
            w(1)
    credit(0)
    kv_start(0, pl.ds(0, SEQ), range(NX))
    w(2)
    for t in TWO:
        for p in TWO:
            mlp_in(t, p)
            if t + p < 2:
                w(1)
    credit(1)
    credit(2)
    w(1)
    for t in TWO:
        for side in TWO:
            mlp_out(t, side)
            ring0(t, side)
            if t + side == 0:
                units_start(1)
                w(1)
            else:
                w(1 - t)
        mlp_sent(t)
    credit(LAST)
    for (t, step), n in zip(((0, 1), (1, 1), (0, 2), (1, 2)), (3, 3, 3, 3)):
        w(n)
        ring(t, step)
    w(3)
    finish(0, 0)
    w(2)
    finish(1, 0)
    kv_sent(0)
    a2()
    attend(0, 0, 0, 1)
    mlp_in(0, 0, 0, 2)
    a1()
    b0()
    w(1)
    a3()
    attend(0, 0, 1, 2)
    mlp_in(0, 0, 2, 2)
    w(1)
    a4()
    a5()
    attend(0, 1)
    w(1)
    b1()
    kv_start(1, tok[0], near)
    mlp_in(0, 1)
    w(2)
    for side in TWO:
        mlp_out(0, side)
        ring0(0, side)
    kv_start(1, tok[0], far)
    for fn in b_rest:
        fn()
    attend(1, 0)
    attend(1, 1)
    ring(0, 1)
    mlp_in(1, 0)
    mlp_in(1, 1)
    mlp_sent(0)
    kv_start(1, tok[1], near)
    mlp_out(1, 0)
    ring0(1, 0)
    ring(0, 2)
    mlp_out(1, 1)
    ring0(1, 1)
    ring(1, 1)
    finish(0, 1)
    ring(1, 2)
    kv_start(1, tok[1], far)
    finish(1, 1)
    mlp_sent(1)
    kv_sent(1)
    for layer in TWO:
        for i, ref in enumerate((kc_ref, vc_ref)):
            got = ref.at[layer, pl.ds(0, 2 * GC - 2)]
            pltpu.make_async_remote_copy(src_ref=got, dst_ref=got, send_sem=kv_send, recv_sem=kv_recv.at[layer, i],
                                         device_id=dev_x(0, 1), device_id_type=MESH).wait_recv()


def solution(mesh):
    tok_spec = P(("dp", "row", "col"))
    both = ("row", "col")
    col_spec = P(None, None, both)
    row_spec = P(None, both, None)

    def device_fn(hidden, positions, segments, ln_weight, w_qkv, w_out, w_gate, w_up, w_down):
        layers = w_qkv.shape[0]
        wq = w_qkv.transpose(0, 2, 1).reshape(layers, 3, UNIT, DIM)
        wg = w_gate.transpose(0, 2, 1).reshape(layers, NX, UNIT, DIM)
        wu = w_up.transpose(0, 2, 1).reshape(layers, NX, UNIT, DIM)
        wd = w_down.reshape(layers, NX, UNIT, DIM)

        inv_freq = ROPE_BASE ** (-2.0 * jnp.arange(HEAD_DIM // 2, dtype=F32) / HEAD_DIM)
        pos = positions[0].astype(F32)[:, None]
        angles = pos * inv_freq
        cos, sin = jnp.cos(angles), jnp.sin(angles)
        cos2 = jnp.stack([cos, cos], axis=-1).reshape(SEQ, HEAD_DIM)
        sin2 = jnp.stack([-sin, sin], axis=-1).reshape(SEQ, HEAD_DIM)
        tab_own = jnp.concatenate([cos2, sin2, jnp.broadcast_to(pos, (SEQ, HEAD_DIM))], axis=1)

        vm = pl.BlockSpec(memory_space=pltpu.VMEM)
        hb = pl.BlockSpec(memory_space=pl.ANY)
        dma, duo = pltpu.SemaphoreType.DMA, len(TWO)
        cache = jax.ShapeDtypeStruct((layers, 2 * GC, SEQ, HEAD_DIM), BF16)
        x_out, kc, vc, _ = pl.pallas_call(
            kernel,
            out_shape=(jax.ShapeDtypeStruct((SEQ, DIM), BF16), cache, cache, jax.ShapeDtypeStruct((layers, UNITS, UNIT, DIM), BF16)),
            in_specs=[hb] * 6 + [vm, hb],
            out_specs=(vm, hb, hb, hb),
            scratch_shapes=[
                pltpu.VMEM((16, SEQ, DIM), BF16),
                pltpu.VMEM((GC, SEQ, DIM), BF16),
                pltpu.VMEM((GC, SEQ, 3 * LANE), F32),
                pltpu.VMEM((GC, SEQ, SIDE), BF16),
                pltpu.VMEM((GC, SEQ, SEQ), BF16),
                pltpu.VMEM((GC, duo, duo, SEQ, HEAD_DIM), BF16),
                pltpu.VMEM((duo, NX, HT, DIM), F32),
                pltpu.VMEM((NX, HT, DIM), F32),
                pltpu.VMEM((duo, NX, HT, DIM), F32),
                pltpu.VMEM((duo, LAST, HT, SIDE), F32),
                pltpu.VMEM((duo, LAST, HT, SIDE), F32),
                dma((duo,)), dma((duo, UNITS)), dma((NX, duo, 20)), dma((NX,)), dma((NX, duo)), pltpu.SemaphoreType.REGULAR((NX,)),
                dma((duo, GC)), dma((duo, GC)), dma((GC,)), dma((GC,)), dma,
                dma((duo, duo)), dma, dma((duo,)), dma((duo, duo, NX)), dma((duo, NX)), dma((duo, duo, LAST)), dma((duo, duo, LAST)),
            ],
            compiler_params=pltpu.CompilerParams(collective_id=0, has_side_effects=True, vmem_limit_bytes=67043328),
        )(wq, wg, wu, wd, w_out, hidden[0], ln_weight.astype(F32), tab_own)
        return x_out[None], kc[None], vc[None]

    return jax.shard_map(device_fn, mesh=mesh, in_specs=(tok_spec, tok_spec, tok_spec, P(), col_spec, row_spec, col_spec, col_spec, row_spec), out_specs=(tok_spec, tok_spec, tok_spec), check_vma=False)
```
